16 devices in a mesh: stage: 2 (over z), expert: 8 (over y, x, core).
Axes of the slice: x: 2, y: 2, z: 2, core: 2. Of those that a mesh axis runs over, the one named last changes fastest.
Arguments:
- w_gate: bfloat16 [2, 16, 2048, 1024], P('stage', 'expert')
- w_up: bfloat16 [2, 16, 2048, 1024], P('stage', 'expert')
- w_down: bfloat16 [2, 16, 1024, 2048], P('stage', 'expert')
- x: bfloat16 [4096, 2048], P(('stage', 'expert'))
- expert_ids: int32 [2, 4096, 8], P(None, ('stage', 'expert'))
- gates: float32 [2, 4096, 8], P(None, ('stage', 'expert'))
Outputs:
- output 1: bfloat16 [2, 16, 2048, 2048], P(None, ('stage', 'expert'))
- output 2: bfloat16 [2, 16, 1024, 2048], P(None, ('stage', 'expert'))
- output 3: float32 [2, 4096, 2048], P(None, ('stage', 'expert'))
All inputs are finite; a program needn't handle non-finite values.
Results may differ from the reference program's by a relative error of at most 0.001.
Values are sent between devices in bfloat16 or wider.
A program may use at most 1 GiB of HBM per device.

```python
import jax
import jax.numpy as jnp
from jax import lax

D = 2048
FF = 1024
TOP = 8
LAYERS = 2
EXPERTS = 16
DEVICES = 16
TOK_DEV = 256

TOKENS = DEVICES * TOK_DEV
CAPACITY = 3 * TOK_DEV * TOP // (2 * EXPERTS)
NORM_EPS = 1e-6


def draw_routes(key):
    mean_load = TOK_DEV * TOP // EXPERTS
    half_load = mean_load // 2
    blocks = LAYERS * DEVICES
    key_shift, key_expert, key_token = jax.random.split(key, 3)
    shifts = jax.random.randint(key_shift, (blocks, EXPERTS // 2), 0, half_load + 1)
    shifts = shifts.at[:, 0].set(half_load)
    counts = jnp.stack([mean_load + shifts, mean_load - shifts], axis=-1).reshape(blocks, EXPERTS)
    run_ends = jnp.cumsum(counts, axis=-1)
    entry = jnp.arange(TOK_DEV * TOP)
    virtual = jnp.sum((entry[None, :, None] >= run_ends[:, None, :]).astype(jnp.int32), axis=-1)
    expert_perm = jax.vmap(lambda sub_key: jax.random.permutation(sub_key, EXPERTS))(jax.random.split(key_expert, blocks))
    labels = jax.vmap(lambda table, index: table[index])(expert_perm, virtual)
    labels = jnp.transpose(labels.reshape(blocks, TOP, TOK_DEV), (0, 2, 1))
    token_perm = jax.vmap(lambda sub_key: jax.random.permutation(sub_key, TOK_DEV))(jax.random.split(key_token, blocks))
    routed = jax.vmap(lambda table, index: table[index])(labels, token_perm)
    return routed.reshape(LAYERS, TOKENS, TOP).astype(jnp.int32)


def setup_inputs(seed: int = 0) -> dict:
    key = jax.random.key(seed)
    key_gate, key_up, key_down, key_x, key_mix, key_route = jax.random.split(key, 6)
    w_gate = (jax.random.normal(key_gate, (LAYERS, EXPERTS, D, FF), jnp.float32) * D ** -0.5).astype(jnp.bfloat16)
    w_up = (jax.random.normal(key_up, (LAYERS, EXPERTS, D, FF), jnp.float32) * D ** -0.5).astype(jnp.bfloat16)
    w_down = (jax.random.normal(key_down, (LAYERS, EXPERTS, FF, D), jnp.float32) * FF ** -0.5).astype(jnp.bfloat16)
    x = jax.random.normal(key_x, (TOKENS, D), jnp.float32).astype(jnp.bfloat16)
    gates = jax.nn.softmax(jax.random.normal(key_mix, (LAYERS, TOKENS, TOP), jnp.float32), axis=-1)
    expert_ids = draw_routes(key_route)
    return {"w_gate": w_gate, "w_up": w_up, "w_down": w_down, "x": x, "expert_ids": expert_ids, "gates": gates}


def expert_layer(hidden, layer_in):
    layer_w13, layer_down, layer_ids, layer_mix = layer_in
    normed = (hidden * lax.rsqrt(jnp.mean(hidden * hidden, axis=-1, keepdims=True) + NORM_EPS)).astype(jnp.bfloat16)
    flat_ids = layer_ids.reshape(-1)
    onehot = (flat_ids[:, None] == jnp.arange(EXPERTS)[None, :]).astype(jnp.int32)
    pair_rank = jnp.sum(onehot * jnp.cumsum(onehot, axis=0), axis=-1) - 1
    rows_per_expert = DEVICES * CAPACITY
    slot_pos = flat_ids * rows_per_expert + pair_rank
    pair_tok = jnp.arange(TOKENS * TOP) // TOP
    buffer = jnp.zeros((EXPERTS * rows_per_expert, D), jnp.bfloat16).at[slot_pos].set(normed[pair_tok])
    buffer = buffer.reshape(EXPERTS, rows_per_expert, D).astype(jnp.float32)
    projected = jnp.einsum("erd,edg->erg", buffer, layer_w13.astype(jnp.float32))
    activated = (jax.nn.silu(projected[..., :FF]) * projected[..., FF:]).astype(jnp.bfloat16)
    expert_out = jnp.einsum("erf,efd->erd", activated.astype(jnp.float32), layer_down.astype(jnp.float32)).astype(jnp.bfloat16)
    picked = expert_out.reshape(EXPERTS * rows_per_expert, D)[slot_pos].astype(jnp.float32).reshape(TOKENS, TOP, D)
    new_hidden = hidden + jnp.sum(layer_mix[..., None] * picked, axis=1)
    return new_hidden, new_hidden


def reference(w_gate, w_up, w_down, x, expert_ids, gates):
    w13 = jnp.concatenate([w_gate, w_up], axis=-1)
    _, hiddens = lax.scan(expert_layer, x.astype(jnp.float32), (w13, w_down, expert_ids, gates))
    return w13, w_down, hiddens
```

```python
import functools

import jax
import jax.numpy as jnp
from jax import lax
from jax.experimental import pallas as pl
from jax.experimental.pallas import tpu as pltpu
from jax.sharding import PartitionSpec as P

NORM_EPS = 1e-6
FLAT = ("stage", "expert")
MESH = pl.DeviceIdType.MESH
F32 = jnp.float32
BF16 = jnp.bfloat16
WEIGHT_CHUNKS = 4
EARLY_PAIRS = 7


def flip(a, b):
    return a + b - 2 * a * b


def moe_kernel(tok, width, ff, w_gate, w_up, w_down, x_ref, gt_ref, w13, wdn, hid, u_all, s_loc, d2d, r1, r2, s_out, fin,
               wv_g, wv_u, wv_d, h, ub, ut, av, pp, ta, gall, gc, hs,
               wsem, lsem, gsem, us, up, ax, af, ap, az, dsend, drecv, s1, q1, s2, q2, so, hr, sw, rw):
    half = width // 2
    tile_f = min(256, ff)
    tile_d = min(256, half)
    lanes = min(128, tok)
    z = lax.axis_index("stage")
    e = lax.axis_index("expert")
    y, x, c = e // 4, (e // 2) % 2, e % 2
    me = z * 8 + e
    ny, nx, nc, nz = 1 - y, 1 - x, 1 - c, 1 - z
    fy, fx = (1 - c) * y + c * ny, (1 - c) * nx + c * x
    sy, sx = c * y + (1 - c) * ny, c * nx + (1 - c) * x

    def dev(dz, dy, dx, dc):
        return (dz, dy * 4 + dx * 2 + dc)

    def group(gz, gy, gx):
        return gz * 4 + gy * 2 + gx

    def remote(src, dst, ssem, rsem, to):
        return pltpu.make_async_remote_copy(src_ref=src, dst_ref=dst, send_sem=ssem, recv_sem=rsem, device_id=to, device_id_type=MESH)

    def local(src, dst, sem):
        cp = pltpu.make_async_copy(src, dst, sem)
        cp.start()
        cp.wait()

    own_gate = pltpu.make_async_copy(gt_ref.at[me], gall.at[me], gsem.at[2])
    own_gate.start()

    def send_gate(off, carry):
        to = lax.rem(me + off, 16)
        remote(gt_ref.at[to], gall.at[me], gsem.at[0], gsem.at[1], (to // 8, lax.rem(to, 8))).start()
        return carry

    lax.fori_loop(1, 16, send_gate, 0)

    own_x = pltpu.make_async_copy(x_ref, ub, lsem.at[0])
    own_x.start()
    w_loads = [pltpu.make_async_copy(w_gate.at[0], wv_g, wsem.at[0]), pltpu.make_async_copy(w_up.at[0], wv_u, wsem.at[1]), pltpu.make_async_copy(w_down.at[0], wv_d, wsem.at[2])]
    for load in w_loads:
        load.start()
    own_x.wait()
    h[...] = ub[...].astype(F32)

    stays = (1 - flip(z, y)) * (1 - flip(y, x)) * (1 - flip(x, c))

    def weight_parts(k, q):
        rows = pl.ds(q * (width // WEIGHT_CHUNKS), width // WEIGHT_CHUNKS)
        rows_d = pl.ds(q * (ff // WEIGHT_CHUNKS), ff // WEIGHT_CHUNKS)
        return ((w_gate.at[0, k, rows], wv_g.at[k, rows], w13.at[z, 0, rows, pl.ds(0, ff)], 0),
                (w_up.at[0, k, rows], wv_u.at[k, rows], w13.at[z, 0, rows, pl.ds(ff, ff)], 0),
                (w_down.at[0, k, rows_d], wv_d.at[k, rows_d], wdn.at[z, 0, rows_d], 1))

    def send_weights(pairs):
        for k, q in pairs:
            is_self = jnp.logical_and(stays == 1, c == k)

            @pl.when(is_self)
            def _():
                for _, src, dst, kind in weight_parts(k, q):
                    pltpu.make_async_copy(src, dst, rw.at[z, kind]).start()

            @pl.when(jnp.logical_not(is_self))
            def _():
                for src, _, dst, kind in weight_parts(k, q):
                    remote(src, dst, sw.at[k, kind], rw.at[z, kind], (y, x * 4 + c * 2 + k)).start()

    pairs = [(k, q) for q in range(WEIGHT_CHUNKS) for k in range(2)]

    def compute(k, slot, gz, gy, gx):
        g = group(gz, gy, gx)
        local(u_all.at[g], ut, lsem.at[0])
        for b in range(2):
            flat = gz * 8 + gy * 4 + gx * 2 + b
            for j in range(tok // lanes):
                row = gall[flat, :, j * lanes:(j + 1) * lanes]
                gc[b * tok + j * lanes:b * tok + (j + 1) * lanes, :] = jnp.concatenate([row] * (lanes // 8), axis=0).T
        for ex in range(2):
            def ff_tile(t, carry):
                cols = pl.ds(pl.multiple_of(t * tile_f, tile_f), tile_f)
                rows_u = ut[...].reshape(2 * tok, width)
                zg = jnp.dot(rows_u, wv_g[ex, :, cols], preferred_element_type=F32)
                zu = jnp.dot(rows_u, wv_u[ex, :, cols], preferred_element_type=F32)
                av[:, cols] = (jax.nn.silu(zg) * zu).astype(BF16)
                return carry

            lax.fori_loop(0, ff // tile_f, ff_tile, 0)

            def out_tile(t, carry):
                cols = pl.ds(pl.multiple_of(t * tile_d, tile_d), tile_d)
                side = t // (half // tile_d)
                at = pl.ds(pl.multiple_of(lax.rem(t, half // tile_d) * tile_d, tile_d), tile_d)
                o = jnp.dot(av[...], wv_d[ex, :, cols], preferred_element_type=F32).astype(BF16).astype(F32)
                gate = gc[:, ex:ex + 1]
                o = jnp.where(gate > 0, gate * o, 0.0)
                for b in range(2):
                    part = o[b * tok:(b + 1) * tok]
                    if ex:
                        part = part + pp[slot, side, b, :, at]
                    pp[slot, side, b, :, at] = part
                return carry

            lax.fori_loop(0, width // tile_d, out_tile, 0)

    def lane(gz, gy, gx):
        return u_all.at[group(gz, gy, gx), c]

    def lane_part(gz, gy, gx, which):
        return u_all.at[group(gz, gy, gx), c, pl.ds(which * (tok // 2), tok // 2)]

    def to_x(d, gz):
        return remote(lane(gz, y, x), lane(gz, y, x), ax.at[d, 0], us.at[d, 0], dev(z, y, nx, c))

    def to_y(d, gz):
        return remote(lane(gz, y, x), lane(gz, y, x), ax.at[d, 1], us.at[d, 1], dev(z, ny, x, c))

    def x_on(d, gz):
        return remote(lane_part(gz, y, nx, 0), lane_part(gz, y, nx, 0), af.at[d, 0], us.at[d, 2], dev(z, ny, x, c))

    def y_on(d, gz):
        return remote(lane_part(gz, ny, x, 1), lane_part(gz, ny, x, 1), af.at[d, 1], us.at[d, 3], dev(z, y, nx, c))

    def to_partner(d, gz, gy, gx, cls):
        return remote(lane(gz, gy, gx), lane(gz, gy, gx), ap.at[d, cls], up.at[d, cls], dev(z, y, x, nc))

    def got(dst, sem):
        pltpu.make_async_copy(dst, dst, sem).wait()

    def to_z(layer_dev):
        return remote(lane(z, y, x), lane(z, y, x), az.at[0], us.at[1, 4], dev(nz, y, x, c))

    def spread(d, gz):
        to_x(d, gz).start()
        to_y(d, gz).start()
        to_partner(d, gz, y, x, 0).start()

    def relay(d, gz):
        got(lane(gz, y, nx), us.at[d, 0])
        x_on(d, gz).start()
        to_partner(d, gz, y, nx, 1).start()
        got(lane(gz, ny, x), us.at[d, 1])
        y_on(d, gz).start()
        to_partner(d, gz, ny, x, 2).start()

    def corner(d, gz):
        got(lane_part(gz, ny, nx, 0), us.at[d, 2])
        got(lane_part(gz, ny, nx, 1), us.at[d, 3])
        to_partner(d, gz, ny, nx, 3).start()

    def d2d_copy(k, slot):
        return remote(pp.at[slot, nc], d2d.at[k], dsend.at[slot], drecv.at[k], dev(z, y, x, nc))

    def step_class(k):
        cls = k // 2
        return lax.rem(k + k // 6, 2), cls // 2, lax.rem(cls, 2)

    def first_send(k, d, ds, b):
        return remote(s_loc.at[k, b], r1.at[d * 2 + ds, b], s1.at[d * 2 + ds, b], q1.at[d * 2 + ds, b], dev(z, fy, fx, c))

    def post(k):
        slot = lax.rem(k, 2)
        d, dy, dx = step_class(k)
        df = (1 - c) * dx + c * dy
        ds = (1 - c) * dy + c * dx
        got(d2d.at[k], drecv.at[k])
        local(d2d.at[k], ta, lsem.at[0])
        for b in range(2):
            pp[slot, c, b] = pp[slot, c, b] + ta[b]
        local(pp.at[slot, c], s_loc.at[k], lsem.at[0])

        @pl.when(df == 1)
        def _():
            for b in range(2):
                first_send(k, d, ds, b).start()

    def second_send(d, b):
        return remote(s_out.at[d, b], r2.at[d, b], s2.at[d, b], q2.at[d, b], dev(z, sy, sx, c))

    def finish_second(d, b):
        k = (2 - c) * 2 + d
        load = pltpu.make_async_copy(s_loc.at[k, b], ta.at[0], lsem.at[0])
        load.start()
        got(r1.at[d * 2 + 1, b], q1.at[d * 2 + 1, b])
        local(r1.at[d * 2 + 1, b], ta.at[1], lsem.at[1])
        load.wait()
        ta[0] = ta[0] + ta[1]
        local(ta.at[0], s_out.at[d, b], lsem.at[0])
        second_send(d, b).start()

    def home_send(d, b):
        return remote(fin.at[d, b], hs.at[z, c], so.at[d, b], hr.at[z, c], dev(flip(z, d), y, x, b))

    def finish_own(d, b):
        load = pltpu.make_async_copy(s_loc.at[d, b], ta.at[0], lsem.at[0])
        load.start()
        got(r1.at[d * 2, b], q1.at[d * 2, b])
        local(r1.at[d * 2, b], ta.at[1], lsem.at[1])
        load.wait()
        ta[0] = ta[0] + ta[1]
        got(r2.at[d, b], q2.at[d, b])
        local(r2.at[d, b], ta.at[1], lsem.at[1])
        ta[0] = ta[0] + ta[1]
        local(ta.at[0], fin.at[d, b], lsem.at[0])
        if d == 1:
            home_send(d, b).start()
        else:
            @pl.when(c == b)
            def _():
                pltpu.make_async_copy(fin.at[d, b], hs.at[z, c], hr.at[z, c]).start()

            @pl.when(c != b)
            def _():
                home_send(d, b).start()

    def active():
        spread(0, z)

        @pl.when(z == 0)
        def _():
            for load in w_loads:
                load.wait()

        own_gate.wait()
        got(gall.at[pl.ds(0, 15)], gsem.at[1])

        def step(k, carry):
            d, dy, dx = step_class(k)
            gz, gy, gx = flip(z, d), flip(y, dy), flip(x, dx)
            cls = k // 2
            slot = lax.rem(k, 2)

            @pl.when(k == 1)
            def _():
                got(lane(nz, y, x), us.at[1, 4])
                spread(1, nz)

            @pl.when(k == 2)
            def _():
                relay(0, z)

            @pl.when(k == 3)
            def _():
                relay(1, nz)

            @pl.when(k == 4)
            def _():
                corner(0, z)

            @pl.when(k == 5)
            def _():
                corner(1, nz)

            got(u_all.at[group(gz, gy, gx), nc], up.at[d, cls])

            @pl.when(k >= 2)
            def _():
                d2d_copy(k - 2, slot).wait_send()

            compute(k, slot, gz, gy, gx)
            d2d_copy(k, slot).start()

            @pl.when(k >= 1)
            def _():
                post(k - 1)

            return carry

        lax.fori_loop(0, 8, step, 0)
        post(7)
        for d in (1, 0):
            for b in range(2):
                finish_second(d, b)
        for d in (1, 0):
            for b in range(2):
                finish_own(d, b)

    def drain():
        for d in range(2):
            gz = flip(z, d)
            to_x(d, gz).wait_send()
            to_y(d, gz).wait_send()
            x_on(d, gz).wait_send()
            y_on(d, gz).wait_send()
            for cls in range(4):
                to_partner(d, gz, flip(y, cls // 2), flip(x, cls % 2), cls).wait_send()
            d2d_copy(6 + d, d).wait_send()
            for b in range(2):
                for ds in range(2):
                    first_send(0, d, ds, b).wait_send()
                second_send(d, b).wait_send()
            for b in range(2):
                if d == 1:
                    home_send(d, b).wait_send()
                else:
                    @pl.when(c != b)
                    def _():
                        home_send(d, b).wait_send()

    def layer(l, carry):
        rows = min(32, tok)

        def norm(i, cc):
            r = pl.ds(pl.multiple_of(i * rows, rows), rows)
            v = h[r, :]
            ub[r, :] = (v * lax.rsqrt(jnp.mean(v * v, axis=-1, keepdims=True) + NORM_EPS)).astype(BF16)
            return cc

        lax.fori_loop(0, tok // rows, norm, 0)
        local(ub, lane(z, y, x), lsem.at[0])

        @pl.when(z != l)
        def _():
            to_z(l).start()

            @pl.when(z == 1)
            def _():
                for load in w_loads:
                    load.wait()
                send_weights(pairs[:EARLY_PAIRS])

            @pl.when(z == 0)
            def _():
                send_weights(pairs)

        @pl.when(z == l)
        def _():
            active()

            @pl.when(z == 1)
            def _():
                send_weights(pairs[EARLY_PAIRS:])

        for s in range(2):
            got(hs.at[l, s], hr.at[l, s])
            h[:, s * half:(s + 1) * half] = h[:, s * half:(s + 1) * half] + hs[l, s]
        local(h, hid.at[l], lsem.at[0])

        @pl.when(z == l)
        def _():
            drain()

        @pl.when(z != l)
        def _():
            to_z(l).wait_send()

        return carry

    lax.fori_loop(0, 2, layer, 0)

    got(gt_ref.at[pl.ds(0, 15)], gsem.at[0])
    for k in range(2):
        @pl.when(jnp.logical_not(jnp.logical_and(stays == 1, c == k)))
        def _():
            got(w13.at[0], sw.at[k, 0])
            got(wdn.at[0], sw.at[k, 1])
    for s in range(2):
        got(w13.at[s], rw.at[s, 0])
        got(wdn.at[s], rw.at[s, 1])


def solution(mesh):
    n_experts = mesh.shape["stage"] * mesh.shape["expert"]

    def per_device(gate_loc, up_loc, down_loc, x_loc, ids_loc, mix_loc):
        tok, width = x_loc.shape
        ff = gate_loc.shape[-1]
        half = width // 2
        chosen = ids_loc[..., None] == jnp.arange(n_experts)
        table = jnp.sum(jnp.where(chosen, mix_loc[..., None], 0.0), axis=2)
        table = jnp.transpose(table, (0, 2, 1)).reshape(16, 2, tok)
        table = jnp.pad(table, ((0, 0), (0, 6), (0, 0)))
        hbm = pl.BlockSpec(memory_space=pl.ANY)
        sds = jax.ShapeDtypeStruct
        outs = pl.pallas_call(
            functools.partial(moe_kernel, tok, width, ff),
            out_shape=(
                sds((2, 1, width, 2 * ff), BF16), sds((2, 1, ff, width), BF16), sds((2, tok, width), F32),
                sds((8, 2, tok, width), BF16),
                sds((8, 2, tok, half), F32), sds((8, 2, tok, half), F32),
                sds((4, 2, tok, half), F32), sds((2, 2, tok, half), F32), sds((2, 2, tok, half), F32), sds((2, 2, tok, half), F32),
            ),
            in_specs=[hbm] * 5,
            out_specs=(hbm,) * 10,
            scratch_shapes=[
                pltpu.VMEM((2, width, ff), BF16), pltpu.VMEM((2, width, ff), BF16), pltpu.VMEM((2, ff, width), BF16),
                pltpu.VMEM((tok, width), F32), pltpu.VMEM((tok, width), BF16),
                pltpu.VMEM((2, tok, width), BF16), pltpu.VMEM((2 * tok, ff), BF16),
                pltpu.VMEM((2, 2, 2, tok, half), F32), pltpu.VMEM((2, tok, half), F32),
                pltpu.VMEM((16, 8, tok), F32), pltpu.VMEM((2 * tok, min(128, tok)), F32), pltpu.VMEM((2, 2, tok, half), F32),
            ] + [pltpu.SemaphoreType.DMA(s) for s in (
                (3,), (2,), (3,), (2, 5), (2, 4), (2, 2), (2, 2), (2, 4), (1,),
                (2,), (8,), (4, 2), (4, 2), (2, 2), (2, 2), (2, 2), (2, 2), (2, 2), (2, 2))],
            compiler_params=pltpu.CompilerParams(has_side_effects=True, vmem_limit_bytes=66_000_000),
        )(gate_loc, up_loc, down_loc, x_loc, table)
        return outs[0], outs[1], outs[2]

    weight_spec = P("stage", "expert")
    token_spec = P(None, FLAT)
    return jax.shard_map(per_device, mesh=mesh, in_specs=(weight_spec, weight_spec, weight_spec, P(FLAT), token_spec, token_spec), out_specs=(token_spec, token_spec, token_spec), check_vma=False)
```

```python
import functools

import jax
import jax.numpy as jnp
from jax import lax
from jax.experimental import pallas as pl
from jax.experimental.pallas import tpu as pltpu
from jax.sharding import PartitionSpec as P

NORM_EPS = 1e-6
FLAT = ("stage", "expert")
MESH = pl.DeviceIdType.MESH
F32 = jnp.float32
BF16 = jnp.bfloat16
WEIGHT_CHUNKS = 4
AHEAD = 2
EARLY_PAIRS = 8
ORDER = ((0, 0), (0, 1), (1, 1), (1, 2), (1, 3), (0, 2), (1, 0), (0, 3))
STEP = {group: k for k, group in enumerate(ORDER)}
TABLE = sum((4 * d + cls) * 8 ** k for k, (d, cls) in enumerate(ORDER))


def flip(a, b):
    return a + b - 2 * a * b


def moe_kernel(tok, width, ff, w_gate, w_up, w_down, x_ref, gt_ref, w13, wdn, hid, u_all, s_loc, d2d, r1, r2, s_out, fin,
               wv_g, wv_u, wv_d, h, ub, ut, av, pp, ta, gall, gc, hs,
               wsem, lsem, gsem, us, up, ax, af, ap, az, dsend, drecv, s1, q1, s2, q2, so, hr, sw, rw, plane):
    half = width // 2
    tile_f = min(512, ff)
    tile_d = min(512, half)
    lanes = min(128, tok)
    z = lax.axis_index("stage")
    e = lax.axis_index("expert")
    y, x, c = e // 4, (e // 2) % 2, e % 2
    me = z * 8 + e
    ny, nx, nc, nz = 1 - y, 1 - x, 1 - c, 1 - z
    fy, fx = (1 - c) * y + c * ny, (1 - c) * nx + c * x
    sy, sx = c * y + (1 - c) * ny, c * nx + (1 - c) * x

    def dev(dz, dy, dx, dc):
        return (dz, dy * 4 + dx * 2 + dc)

    def group(gz, gy, gx):
        return gz * 4 + gy * 2 + gx

    def remote(src, dst, ssem, rsem, to):
        return pltpu.make_async_remote_copy(src_ref=src, dst_ref=dst, send_sem=ssem, recv_sem=rsem, device_id=to, device_id_type=MESH)

    def local(src, dst, sem):
        cp = pltpu.make_async_copy(src, dst, sem)
        cp.start()
        cp.wait()

    own_gate = pltpu.make_async_copy(gt_ref.at[me], gall.at[me], gsem.at[2])
    own_gate.start()

    def send_gate(off, carry):
        to = lax.rem(me + off, 16)
        remote(gt_ref.at[to], gall.at[me], gsem.at[0], gsem.at[1], (to // 8, lax.rem(to, 8))).start()
        return carry

    lax.fori_loop(1, 16, send_gate, 0)

    own_x = pltpu.make_async_copy(x_ref, ub, lsem.at[0])
    own_x.start()
    w_loads = [pltpu.make_async_copy(w_gate.at[0], wv_g, wsem.at[0]), pltpu.make_async_copy(w_up.at[0], wv_u, wsem.at[1]), pltpu.make_async_copy(w_down.at[0], wv_d, wsem.at[2])]
    for load in w_loads:
        load.start()
    own_x.wait()
    h[...] = ub[...].astype(F32)

    stays = (1 - flip(z, y)) * (1 - flip(y, x)) * (1 - flip(x, c))

    def weight_parts(k, q):
        rows = pl.ds(q * (width // WEIGHT_CHUNKS), width // WEIGHT_CHUNKS)
        rows_d = pl.ds(q * (ff // WEIGHT_CHUNKS), ff // WEIGHT_CHUNKS)
        return ((w_gate.at[0, k, rows], wv_g.at[k, rows], w13.at[z, 0, rows, pl.ds(0, ff)], 0),
                (w_up.at[0, k, rows], wv_u.at[k, rows], w13.at[z, 0, rows, pl.ds(ff, ff)], 0),
                (w_down.at[0, k, rows_d], wv_d.at[k, rows_d], wdn.at[z, 0, rows_d], 1))

    def stays_here(k):
        return jnp.logical_and(stays == 1, c == k)

    def weight_copies(k, q):
        return [remote(src, dst, sw.at[k, q, i], rw.at[z, kind], (y, x * 4 + c * 2 + k))
                for i, (src, _, dst, kind) in enumerate(weight_parts(k, q))]

    def send_weights(pairs):
        for k, q in pairs:
            @pl.when(stays_here(k))
            def _():
                for _, src, dst, kind in weight_parts(k, q):
                    pltpu.make_async_copy(src, dst, rw.at[z, kind]).start()

            @pl.when(jnp.logical_not(stays_here(k)))
            def _():
                for copy in weight_copies(k, q):
                    copy.start()

    def sent_weights(pairs):
        for k, q in pairs:
            @pl.when(jnp.logical_not(stays_here(k)))
            def _():
                for copy in weight_copies(k, q):
                    copy.wait_send()

    def paced_weights(pairs):
        for i, pair in enumerate(pairs):
            send_weights([pair])
            if i >= AHEAD:
                sent_weights([pairs[i - AHEAD]])
        sent_weights(pairs[max(0, len(pairs) - AHEAD):])

    pairs = [(k, q) for q in range(WEIGHT_CHUNKS) for k in range(2)]

    def rows_load(gz, gy, gx):
        return pltpu.make_async_copy(u_all.at[group(gz, gy, gx)], ut, lsem.at[2])

    def gate_columns(gz, gy, gx):
        for b in range(2):
            flat = gz * 8 + gy * 4 + gx * 2 + b
            for j in range(tok // lanes):
                row = gall[flat, :, j * lanes:(j + 1) * lanes]
                gc[b * tok + j * lanes:b * tok + (j + 1) * lanes, :] = jnp.concatenate([row] * (lanes // 8), axis=0).T

    def expert(ex, slot):
        if True:
            def ff_tile(t, carry):
                cols = pl.ds(pl.multiple_of(t * tile_f, tile_f), tile_f)
                rows_u = ut[...].reshape(2 * tok, width)
                zg = jnp.dot(rows_u, wv_g[ex, :, cols], preferred_element_type=F32)
                zu = jnp.dot(rows_u, wv_u[ex, :, cols], preferred_element_type=F32)
                av[:, cols] = (jax.nn.silu(zg) * zu).astype(BF16)
                return carry

            lax.fori_loop(0, ff // tile_f, ff_tile, 0)

            def out_tile(t, carry):
                cols = pl.ds(pl.multiple_of(t * tile_d, tile_d), tile_d)
                side = t // (half // tile_d)
                at = pl.ds(pl.multiple_of(lax.rem(t, half // tile_d) * tile_d, tile_d), tile_d)
                o = jnp.dot(av[...], wv_d[ex, :, cols], preferred_element_type=F32).astype(BF16).astype(F32)
                gate = gc[:, ex:ex + 1]
                o = jnp.where(gate > 0, gate * o, 0.0)
                for b in range(2):
                    part = o[b * tok:(b + 1) * tok]
                    if ex:
                        part = part + pp[slot, side, b, :, at]
                    pp[slot, side, b, :, at] = part
                return carry

            lax.fori_loop(0, width // tile_d, out_tile, 0)

    def lane(gz, gy, gx):
        return u_all.at[group(gz, gy, gx), c]

    def lane_part(gz, gy, gx, which):
        return u_all.at[group(gz, gy, gx), c, pl.ds(which * (tok // 2), tok // 2)]

    def to_x(d, gz):
        return remote(lane(gz, y, x), lane(gz, y, x), ax.at[d, 0], us.at[d, 0], dev(z, y, nx, c))

    def to_y(d, gz):
        return remote(lane(gz, y, x), lane(gz, y, x), ax.at[d, 1], us.at[d, 1], dev(z, ny, x, c))

    def x_on(d, gz):
        return remote(lane_part(gz, y, nx, 0), lane_part(gz, y, nx, 0), af.at[d, 0], us.at[d, 2], dev(z, ny, x, c))

    def y_on(d, gz):
        return remote(lane_part(gz, ny, x, 1), lane_part(gz, ny, x, 1), af.at[d, 1], us.at[d, 3], dev(z, y, nx, c))

    def to_partner(d, gz, gy, gx, cls):
        return remote(lane(gz, gy, gx), lane(gz, gy, gx), ap.at[d, cls], up.at[d, cls], dev(z, y, x, nc))

    def got(dst, sem):
        pltpu.make_async_copy(dst, dst, sem).wait()

    def to_z(layer_dev):
        return remote(lane(z, y, x), lane(z, y, x), az.at[0], us.at[1, 4], dev(nz, y, x, c))

    def spread(d, gz):
        to_x(d, gz).start()
        to_y(d, gz).start()
        to_partner(d, gz, y, x, 0).start()

    def relay(d, gz):
        got(lane(gz, y, nx), us.at[d, 0])
        x_on(d, gz).start()
        to_partner(d, gz, y, nx, 1).start()
        got(lane(gz, ny, x), us.at[d, 1])
        y_on(d, gz).start()
        to_partner(d, gz, ny, x, 2).start()

    def corner(d, gz):
        got(lane_part(gz, ny, nx, 0), us.at[d, 2])
        got(lane_part(gz, ny, nx, 1), us.at[d, 3])
        to_partner(d, gz, ny, nx, 3).start()

    def d2d_copy(k, slot):
        return remote(pp.at[slot, nc], d2d.at[k], dsend.at[slot], drecv.at[k], dev(z, y, x, nc))

    def step_class(k):
        code = lax.rem(lax.div(jnp.int32(TABLE), lax.shift_left(jnp.int32(1), 3 * k)), 8)
        return code // 4, lax.rem(code // 2, 2), lax.rem(code, 2)

    def first_send(k, d, ds, b):
        return remote(s_loc.at[k, b], r1.at[d * 2 + ds, b], s1.at[d * 2 + ds, b], q1.at[d * 2 + ds, b], dev(z, fy, fx, c))

    def sum_load(k):
        return pltpu.make_async_copy(d2d.at[k], ta, lsem.at[3])

    def sum_store(k, slot):
        return pltpu.make_async_copy(pp.at[slot, c], s_loc.at[k], lsem.at[4])

    def add_partner(k, slot):
        sum_load(k).wait()
        for b in range(2):
            pp[slot, c, b] = pp[slot, c, b] + ta[b]
        sum_store(k, slot).start()

    def pass_on(k, slot):
        d, dy, dx = step_class(k)
        df = (1 - c) * dx + c * dy
        ds = (1 - c) * dy + c * dx
        sum_store(k, slot).wait()

        @pl.when(df == 1)
        def _():
            for b in range(2):
                first_send(k, d, ds, b).start()

    def second_send(d, b):
        return remote(s_out.at[d, b], r2.at[d, b], s2.at[d, b], q2.at[d, b], dev(z, sy, sx, c))

    def finish_second(d, b):
        k = c * STEP[d, 1] + (1 - c) * STEP[d, 2]
        load = pltpu.make_async_copy(s_loc.at[k, b], ta.at[0], lsem.at[0])
        load.start()
        got(r1.at[d * 2 + 1, b], q1.at[d * 2 + 1, b])
        local(r1.at[d * 2 + 1, b], ta.at[1], lsem.at[1])
        load.wait()
        ta[0] = ta[0] + ta[1]
        local(ta.at[0], s_out.at[d, b], lsem.at[0])
        second_send(d, b).start()

    def home_send(d, b):
        return remote(fin.at[d, b], hs.at[z, c], so.at[d, b], hr.at[z, c], dev(flip(z, d), y, x, b))

    def finish_own(d, b):
        load = pltpu.make_async_copy(s_loc.at[STEP[d, 0], b], ta.at[0], lsem.at[0])
        load.start()
        got(r1.at[d * 2, b], q1.at[d * 2, b])
        local(r1.at[d * 2, b], ta.at[1], lsem.at[1])
        load.wait()
        ta[0] = ta[0] + ta[1]
        got(r2.at[d, b], q2.at[d, b])
        local(r2.at[d, b], ta.at[1], lsem.at[1])
        ta[0] = ta[0] + ta[1]
        local(ta.at[0], fin.at[d, b], lsem.at[0])
        if d == 1:
            home_send(d, b).start()
        else:
            @pl.when(c == b)
            def _():
                pltpu.make_async_copy(fin.at[d, b], hs.at[z, c], hr.at[z, c]).start()

            @pl.when(c != b)
            def _():
                home_send(d, b).start()

    def active():
        spread(0, z)

        @pl.when(z == 0)
        def _():
            for load in w_loads:
                load.wait()

        own_gate.wait()
        got(gall.at[pl.ds(0, 15)], gsem.at[1])

        def step(k, carry):
            d, dy, dx = step_class(k)
            gz, gy, gx = flip(z, d), flip(y, dy), flip(x, dx)
            cls = dy * 2 + dx
            slot = lax.rem(k, 2)

            @pl.when(k == 1)
            def _():
                got(lane(nz, y, x), us.at[1, 4])
                spread(1, nz)

            for dd in range(2):
                @pl.when(k == max(1, min(STEP[dd, 1], STEP[dd, 2])))
                def _():
                    relay(dd, flip(z, dd))

                @pl.when(k == STEP[dd, 3])
                def _():
                    corner(dd, flip(z, dd))

            got(u_all.at[group(gz, gy, gx), nc], up.at[d, cls])
            rows_load(gz, gy, gx).start()
            gate_columns(gz, gy, gx)

            @pl.when(k >= 2)
            def _():
                pass_on(k - 2, slot)
                d2d_copy(k - 2, slot).wait_send()

            rows_load(gz, gy, gx).wait()
            expert(0, slot)

            @pl.when(k == 7)
            def _():
                for b in range(2):
                    finish_second(1, b)

            @pl.when(k >= 1)
            def _():
                got(d2d.at[k - 1], drecv.at[k - 1])
                sum_load(k - 1).start()

            expert(1, slot)

            @pl.when(k >= 1)
            def _():
                add_partner(k - 1, 1 - slot)

            d2d_copy(k, slot).start()
            return carry

        lax.fori_loop(0, 8, step, 0)
        pass_on(6, 0)
        got(d2d.at[7], drecv.at[7])
        sum_load(7).start()
        add_partner(7, 1)
        pass_on(7, 1)
        for b in range(2):
            finish_own(1, b)
        for b in range(2):
            finish_second(0, b)
        for b in range(2):
            finish_own(0, b)

    def drain():
        for d in range(2):
            gz = flip(z, d)
            to_x(d, gz).wait_send()
            to_y(d, gz).wait_send()
            x_on(d, gz).wait_send()
            y_on(d, gz).wait_send()
            for cls in range(4):
                to_partner(d, gz, flip(y, cls // 2), flip(x, cls % 2), cls).wait_send()
            d2d_copy(6 + d, d).wait_send()
            for b in range(2):
                for ds in range(2):
                    first_send(0, d, ds, b).wait_send()
                second_send(d, b).wait_send()
            for b in range(2):
                if d == 1:
                    home_send(d, b).wait_send()
                else:
                    @pl.when(c != b)
                    def _():
                        home_send(d, b).wait_send()

    def layer(l, carry):
        rows = min(32, tok)

        def norm(i, cc):
            r = pl.ds(pl.multiple_of(i * rows, rows), rows)
            v = h[r, :]
            ub[r, :] = (v * lax.rsqrt(jnp.mean(v * v, axis=-1, keepdims=True) + NORM_EPS)).astype(BF16)
            return cc

        lax.fori_loop(0, tok // rows, norm, 0)
        local(ub, lane(z, y, x), lsem.at[0])

        @pl.when(z != l)
        def _():
            to_z(l).start()
            to_z(l).wait_send()
            for i in range(1, 8):
                pl.semaphore_signal(plane, inc=1, device_id=(z, lax.rem(e + i, 8)), device_id_type=MESH)
            pl.semaphore_wait(plane, 7)

            @pl.when(z == 1)
            def _():
                for load in w_loads:
                    load.wait()
                send_weights(pairs[:EARLY_PAIRS])

            @pl.when(z == 0)
            def _():
                send_weights(pairs)

        @pl.when(z == l)
        def _():
            active()

            @pl.when(z == 1)
            def _():
                send_weights(pairs[EARLY_PAIRS:])

        for s in range(2):
            got(hs.at[l, s], hr.at[l, s])
            h[:, s * half:(s + 1) * half] = h[:, s * half:(s + 1) * half] + hs[l, s]
        local(h, hid.at[l], lsem.at[0])

        @pl.when(z == l)
        def _():
            drain()

        return carry

    lax.fori_loop(0, 2, layer, 0)

    got(gt_ref.at[pl.ds(0, 15)], gsem.at[0])
    @pl.when(z == 0)
    def _():
        sent_weights(pairs)

    @pl.when(z == 1)
    def _():
        sent_weights(pairs)

    for s in range(2):
        got(w13.at[s], rw.at[s, 0])
        got(wdn.at[s], rw.at[s, 1])


def solution(mesh):
    n_experts = mesh.shape["stage"] * mesh.shape["expert"]

    def per_device(gate_loc, up_loc, down_loc, x_loc, ids_loc, mix_loc):
        tok, width = x_loc.shape
        ff = gate_loc.shape[-1]
        half = width // 2
        chosen = ids_loc[..., None] == jnp.arange(n_experts)
        table = jnp.sum(jnp.where(chosen, mix_loc[..., None], 0.0), axis=2)
        table = jnp.transpose(table, (0, 2, 1)).reshape(16, 2, tok)
        table = jnp.pad(table, ((0, 0), (0, 6), (0, 0)))
        hbm = pl.BlockSpec(memory_space=pl.ANY)
        sds = jax.ShapeDtypeStruct
        outs = pl.pallas_call(
            functools.partial(moe_kernel, tok, width, ff),
            out_shape=(
                sds((2, 1, width, 2 * ff), BF16), sds((2, 1, ff, width), BF16), sds((2, tok, width), F32),
                sds((8, 2, tok, width), BF16),
                sds((8, 2, tok, half), F32), sds((8, 2, tok, half), F32),
                sds((4, 2, tok, half), F32), sds((2, 2, tok, half), F32), sds((2, 2, tok, half), F32), sds((2, 2, tok, half), F32),
            ),
            in_specs=[hbm] * 5,
            out_specs=(hbm,) * 10,
            scratch_shapes=[
                pltpu.VMEM((2, width, ff), BF16), pltpu.VMEM((2, width, ff), BF16), pltpu.VMEM((2, ff, width), BF16),
                pltpu.VMEM((tok, width), F32), pltpu.VMEM((tok, width), BF16),
                pltpu.VMEM((2, tok, width), BF16), pltpu.VMEM((2 * tok, ff), BF16),
                pltpu.VMEM((2, 2, 2, tok, half), F32), pltpu.VMEM((2, tok, half), F32),
                pltpu.VMEM((16, 8, tok), F32), pltpu.VMEM((2 * tok, min(128, tok)), F32), pltpu.VMEM((2, 2, tok, half), F32),
            ] + [pltpu.SemaphoreType.DMA(s) for s in (
                (3,), (5,), (3,), (2, 5), (2, 4), (2, 2), (2, 2), (2, 4), (1,),
                (2,), (8,), (4, 2), (4, 2), (2, 2), (2, 2), (2, 2), (2, 2), (2, WEIGHT_CHUNKS, 3), (2, 2))] + [pltpu.SemaphoreType.REGULAR],
            compiler_params=pltpu.CompilerParams(has_side_effects=True, vmem_limit_bytes=66_000_000),
        )(gate_loc, up_loc, down_loc, x_loc, table)
        return outs[0], outs[1], outs[2]

    weight_spec = P("stage", "expert")
    token_spec = P(None, FLAT)
    return jax.shard_map(per_device, mesh=mesh, in_specs=(weight_spec, weight_spec, weight_spec, P(FLAT), token_spec, token_spec), out_specs=(token_spec, token_spec, token_spec), check_vma=False)
```

```python
import functools

import jax
import jax.numpy as jnp
from jax import lax
from jax.experimental import pallas as pl
from jax.experimental.pallas import tpu as pltpu
from jax.sharding import PartitionSpec as P

NORM_EPS = 1e-6
FLAT = ("stage", "expert")
MESH = pl.DeviceIdType.MESH
F32 = jnp.float32
BF16 = jnp.bfloat16
WEIGHT_CHUNKS = 8
COPY_STEPS = 8
GAPS_STAY = (2,)
GAPS_LEAVE = (2, 3)
ORDER = ((0, 0), (0, 1), (1, 1), (1, 3), (1, 2), (0, 3), (0, 2), (1, 0))
STEP = {group: k for k, group in enumerate(ORDER)}
TABLE = sum((4 * d + cls) * 8 ** k for k, (d, cls) in enumerate(ORDER))


def flip(a, b):
    return a + b - 2 * a * b


def moe_kernel(tok, width, ff, w_gate, w_up, w_down, x_ref, gt_ref, w13, wdn, hid, u_all, s_loc, d2d, r1, r2, s_out, fin,
               wv_g, wv_u, wv_d, h, ub, ut, av, pp, ta, gall, gc, hs,
               wsem, lsem, gsem, us, up, ax, af, ap, az, dsend, drecv, s1, q1, s2, q2, so, hr, sw, rw, plane):
    half = width // 2
    tile_f = min(1024, ff)
    tile_d = min(1024, half)
    lanes = min(128, tok)
    z = lax.axis_index("stage")
    e = lax.axis_index("expert")
    y, x, c = e // 4, (e // 2) % 2, e % 2
    me = z * 8 + e
    ny, nx, nc, nz = 1 - y, 1 - x, 1 - c, 1 - z
    fy, fx = (1 - c) * y + c * ny, (1 - c) * nx + c * x
    sy, sx = c * y + (1 - c) * ny, c * nx + (1 - c) * x

    def dev(dz, dy, dx, dc):
        return (dz, dy * 4 + dx * 2 + dc)

    def group(gz, gy, gx):
        return gz * 4 + gy * 2 + gx

    def remote(src, dst, ssem, rsem, to):
        return pltpu.make_async_remote_copy(src_ref=src, dst_ref=dst, send_sem=ssem, recv_sem=rsem, device_id=to, device_id_type=MESH)

    def local(src, dst, sem):
        cp = pltpu.make_async_copy(src, dst, sem)
        cp.start()
        cp.wait()

    own_gate = pltpu.make_async_copy(gt_ref.at[me], gall.at[me], gsem.at[2])
    own_gate.start()

    def send_gate(off, carry):
        to = lax.rem(me + off, 16)
        remote(gt_ref.at[to], gall.at[me], gsem.at[0], gsem.at[1], (to // 8, lax.rem(to, 8))).start()
        return carry

    lax.fori_loop(1, 16, send_gate, 0)

    own_x = pltpu.make_async_copy(x_ref, ub, lsem.at[0])
    own_x.start()
    w_loads = [pltpu.make_async_copy(w_gate.at[0], wv_g, wsem.at[0]), pltpu.make_async_copy(w_up.at[0], wv_u, wsem.at[1]), pltpu.make_async_copy(w_down.at[0], wv_d, wsem.at[2])]
    own_x.wait()
    for load in w_loads:
        load.start()
    h[...] = ub[...].astype(F32)

    stays = (1 - flip(z, y)) * (1 - flip(y, x)) * (1 - flip(x, c))

    def weight_parts(k, q):
        rows = pl.ds(q * (width // WEIGHT_CHUNKS), width // WEIGHT_CHUNKS)
        rows_d = pl.ds(q * (ff // WEIGHT_CHUNKS), ff // WEIGHT_CHUNKS)
        return ((w_gate.at[0, k, rows], wv_g.at[k, rows], w13.at[z, 0, rows, pl.ds(0, ff)], 0),
                (w_up.at[0, k, rows], wv_u.at[k, rows], w13.at[z, 0, rows, pl.ds(ff, ff)], 0),
                (w_down.at[0, k, rows_d], wv_d.at[k, rows_d], wdn.at[z, 0, rows_d], 1))

    def stays_here(k):
        return jnp.logical_and(stays == 1, c == k)

    def weight_copies(k, q):
        return [remote(src, dst, sw.at[k, q, i], rw.at[z, kind], (y, x * 4 + c * 2 + k))
                for i, (src, _, dst, kind) in enumerate(weight_parts(k, q))]

    def send_weights(pairs):
        for k, q in pairs:
            @pl.when(stays_here(k))
            def _():
                for _, src, dst, kind in weight_parts(k, q):
                    pltpu.make_async_copy(src, dst, rw.at[z, kind]).start()

            @pl.when(jnp.logical_not(stays_here(k)))
            def _():
                for copy in weight_copies(k, q):
                    copy.start()

    def sent_weights(pairs):
        for k, q in pairs:
            @pl.when(jnp.logical_not(stays_here(k)))
            def _():
                for copy in weight_copies(k, q):
                    copy.wait_send()

    pairs = [(k, q) for q in range(WEIGHT_CHUNKS) for k in range(2)]
    leaves = flip(y, z) == 1

    def rows_load(gz, gy, gx):
        return pltpu.make_async_copy(u_all.at[group(gz, gy, gx)], ut, lsem.at[2])

    def gate_columns(gz, gy, gx):
        for b in range(2):
            flat = gz * 8 + gy * 4 + gx * 2 + b
            for j in range(tok // lanes):
                row = gall[flat, :, j * lanes:(j + 1) * lanes]
                gc[b * tok + j * lanes:b * tok + (j + 1) * lanes, :] = jnp.concatenate([row] * (lanes // 8), axis=0).T

    def expert(ex, slot):
        if True:
            def ff_tile(t, carry):
                cols = pl.ds(pl.multiple_of(t * tile_f, tile_f), tile_f)
                rows_u = ut[...].reshape(2 * tok, width)
                zg = jnp.dot(rows_u, wv_g[ex, :, cols], preferred_element_type=F32)
                zu = jnp.dot(rows_u, wv_u[ex, :, cols], preferred_element_type=F32)
                av[:, cols] = (jax.nn.silu(zg) * zu).astype(BF16)
                return carry

            lax.fori_loop(0, ff // tile_f, ff_tile, 0)

            def out_tile(t, carry):
                cols = pl.ds(pl.multiple_of(t * tile_d, tile_d), tile_d)
                side = t // (half // tile_d)
                at = pl.ds(pl.multiple_of(lax.rem(t, half // tile_d) * tile_d, tile_d), tile_d)
                o = jnp.dot(av[...], wv_d[ex, :, cols], preferred_element_type=F32).astype(BF16).astype(F32)
                gate = gc[:, ex:ex + 1]
                o = jnp.where(gate > 0, gate * o, 0.0)
                for b in range(2):
                    part = o[b * tok:(b + 1) * tok]
                    if ex:
                        part = part + pp[slot, side, b, :, at]
                    pp[slot, side, b, :, at] = part
                return carry

            lax.fori_loop(0, width // tile_d, out_tile, 0)

    def lane(gz, gy, gx):
        return u_all.at[group(gz, gy, gx), c]

    def lane_part(gz, gy, gx, which):
        return u_all.at[group(gz, gy, gx), c, pl.ds(which * (tok // 2), tok // 2)]

    def to_x(d, gz):
        return remote(lane(gz, y, x), lane(gz, y, x), ax.at[d, 0], us.at[d, 0], dev(z, y, nx, c))

    def to_y(d, gz):
        return remote(lane(gz, y, x), lane(gz, y, x), ax.at[d, 1], us.at[d, 1], dev(z, ny, x, c))

    def x_on(d, gz):
        return remote(lane_part(gz, y, nx, 0), lane_part(gz, y, nx, 0), af.at[d, 0], us.at[d, 2], dev(z, ny, x, c))

    def y_on(d, gz):
        return remote(lane_part(gz, ny, x, 1), lane_part(gz, ny, x, 1), af.at[d, 1], us.at[d, 3], dev(z, y, nx, c))

    def to_partner(d, gz, gy, gx, cls):
        return remote(lane(gz, gy, gx), lane(gz, gy, gx), ap.at[d, cls], up.at[d, cls], dev(z, y, x, nc))

    def got(dst, sem):
        pltpu.make_async_copy(dst, dst, sem).wait()

    def to_z(layer_dev):
        return remote(lane(z, y, x), lane(z, y, x), az.at[0], us.at[1, 4], dev(nz, y, x, c))

    def spread(d, gz):
        to_x(d, gz).start()
        to_y(d, gz).start()
        to_partner(d, gz, y, x, 0).start()

    def relay(d, gz):
        got(lane(gz, y, nx), us.at[d, 0])
        x_on(d, gz).start()
        to_partner(d, gz, y, nx, 1).start()
        got(lane(gz, ny, x), us.at[d, 1])
        y_on(d, gz).start()
        to_partner(d, gz, ny, x, 2).start()

    def corner(d, gz):
        got(lane_part(gz, ny, nx, 0), us.at[d, 2])
        got(lane_part(gz, ny, nx, 1), us.at[d, 3])
        to_partner(d, gz, ny, nx, 3).start()

    def d2d_copy(k, slot):
        return remote(pp.at[slot, nc], d2d.at[k], dsend.at[slot], drecv.at[k], dev(z, y, x, nc))

    def step_class(k):
        code = lax.rem(lax.div(jnp.int32(TABLE), lax.shift_left(jnp.int32(1), 3 * k)), 8)
        return code // 4, lax.rem(code // 2, 2), lax.rem(code, 2)

    def first_send(k, d, ds, b):
        return remote(s_loc.at[k, b], r1.at[d * 2 + ds, b], s1.at[d * 2 + ds, b], q1.at[d * 2 + ds, b], dev(z, fy, fx, c))

    def sum_load(k):
        return pltpu.make_async_copy(d2d.at[k], ta, lsem.at[3])

    def sum_store(k, slot):
        return pltpu.make_async_copy(pp.at[slot, c], s_loc.at[k], lsem.at[4])

    def add_partner(k, slot):
        sum_load(k).wait()
        for b in range(2):
            pp[slot, c, b] = pp[slot, c, b] + ta[b]
        sum_store(k, slot).start()

    def pass_on(k, slot):
        d, dy, dx = step_class(k)
        df = (1 - c) * dx + c * dy
        ds = (1 - c) * dy + c * dx
        sum_store(k, slot).wait()

        @pl.when(df == 1)
        def _():
            for b in range(2):
                first_send(k, d, ds, b).start()

    def second_send(d, b):
        return remote(s_out.at[d, b], r2.at[d, b], s2.at[d, b], q2.at[d, b], dev(z, sy, sx, c))

    def finish_second(d, b):
        k = c * STEP[d, 1] + (1 - c) * STEP[d, 2]
        load = pltpu.make_async_copy(s_loc.at[k, b], ta.at[0], lsem.at[0])
        load.start()
        got(r1.at[d * 2 + 1, b], q1.at[d * 2 + 1, b])
        local(r1.at[d * 2 + 1, b], ta.at[1], lsem.at[1])
        load.wait()
        ta[0] = ta[0] + ta[1]
        local(ta.at[0], s_out.at[d, b], lsem.at[0])
        second_send(d, b).start()

    def home_send(d, b):
        return remote(fin.at[d, b], hs.at[z, c], so.at[d, b], hr.at[z, c], dev(flip(z, d), y, x, b))

    def finish_own(d, b):
        load = pltpu.make_async_copy(s_loc.at[STEP[d, 0], b], ta.at[0], lsem.at[0])
        load.start()
        got(r1.at[d * 2, b], q1.at[d * 2, b])
        local(r1.at[d * 2, b], ta.at[1], lsem.at[1])
        load.wait()
        ta[0] = ta[0] + ta[1]
        got(r2.at[d, b], q2.at[d, b])
        local(r2.at[d, b], ta.at[1], lsem.at[1])
        ta[0] = ta[0] + ta[1]
        local(ta.at[0], fin.at[d, b], lsem.at[0])
        if d == 1:
            home_send(d, b).start()
        else:
            @pl.when(c == b)
            def _():
                pltpu.make_async_copy(fin.at[d, b], hs.at[z, c], hr.at[z, c]).start()

            @pl.when(c != b)
            def _():
                home_send(d, b).start()

    def active():
        spread(0, z)

        @pl.when(z == 0)
        def _():
            for load in w_loads:
                load.wait()

        own_gate.wait()
        got(gall.at[pl.ds(0, 15)], gsem.at[1])

        def step(k, carry):
            d, dy, dx = step_class(k)
            gz, gy, gx = flip(z, d), flip(y, dy), flip(x, dx)
            cls = dy * 2 + dx
            slot = lax.rem(k, 2)

            @pl.when(k == 1)
            def _():
                got(lane(nz, y, x), us.at[1, 4])
                spread(1, nz)

            for dd in range(2):
                @pl.when(k == max(1, min(STEP[dd, 1], STEP[dd, 2])))
                def _():
                    relay(dd, flip(z, dd))

                @pl.when(k == STEP[dd, 3])
                def _():
                    corner(dd, flip(z, dd))

            for mine, gaps in ((jnp.logical_not(leaves), GAPS_STAY), (leaves, GAPS_LEAVE)):
                for pair, at in zip(pairs, gaps):
                    @pl.when(jnp.logical_and(mine, k == at))
                    def _():
                        send_weights([pair])

            got(u_all.at[group(gz, gy, gx), nc], up.at[d, cls])
            rows_load(gz, gy, gx).start()
            gate_columns(gz, gy, gx)

            @pl.when(k >= 2)
            def _():
                pass_on(k - 2, slot)
                d2d_copy(k - 2, slot).wait_send()

            rows_load(gz, gy, gx).wait()
            expert(0, slot)

            @pl.when(k == 7)
            def _():
                for b in range(2):
                    finish_second(1, b)

            @pl.when(k >= 1)
            def _():
                got(d2d.at[k - 1], drecv.at[k - 1])
                sum_load(k - 1).start()

            expert(1, slot)

            @pl.when(k >= 1)
            def _():
                add_partner(k - 1, 1 - slot)

            d2d_copy(k, slot).start()
            return carry

        lax.fori_loop(0, 8, step, 0)
        pass_on(6, 0)
        got(d2d.at[7], drecv.at[7])
        sum_load(7).start()
        add_partner(7, 1)
        pass_on(7, 1)
        for b in range(2):
            finish_own(1, b)
        for b in range(2):
            finish_second(0, b)
        for b in range(2):
            finish_own(0, b)

    def drain():
        for d in range(2):
            gz = flip(z, d)
            to_x(d, gz).wait_send()
            to_y(d, gz).wait_send()
            x_on(d, gz).wait_send()
            y_on(d, gz).wait_send()
            for cls in range(4):
                to_partner(d, gz, flip(y, cls // 2), flip(x, cls % 2), cls).wait_send()
            d2d_copy(6 + d, d).wait_send()
            for b in range(2):
                for ds in range(2):
                    first_send(0, d, ds, b).wait_send()
                second_send(d, b).wait_send()
            for b in range(2):
                if d == 1:
                    home_send(d, b).wait_send()
                else:
                    @pl.when(c != b)
                    def _():
                        home_send(d, b).wait_send()

    def layer(l, carry):
        rows = min(32, tok)

        def norm(i, cc):
            r = pl.ds(pl.multiple_of(i * rows, rows), rows)
            v = h[r, :]
            ub[r, :] = (v * lax.rsqrt(jnp.mean(v * v, axis=-1, keepdims=True) + NORM_EPS)).astype(BF16)
            return cc

        lax.fori_loop(0, tok // rows, norm, 0)
        local(ub, lane(z, y, x), lsem.at[0])

        @pl.when(z != l)
        def _():
            to_z(l).start()

            @pl.when(z == 1)
            def _():
                for load in w_loads:
                    load.wait()

            @pl.when(jnp.logical_not(leaves))
            def _():
                send_weights(pairs[len(GAPS_STAY):])

            to_z(l).wait_send()
            for i in range(1, 8):
                pl.semaphore_signal(plane, inc=1, device_id=(z, lax.rem(e + i, 8)), device_id_type=MESH)
            pl.semaphore_wait(plane, 7)

            @pl.when(leaves)
            def _():
                send_weights(pairs[len(GAPS_LEAVE):])

        @pl.when(z == l)
        def _():
            active()

        for s in range(2):
            got(hs.at[l, s], hr.at[l, s])
            h[:, s * half:(s + 1) * half] = h[:, s * half:(s + 1) * half] + hs[l, s]
        local(h, hid.at[l], lsem.at[0])

        @pl.when(z == l)
        def _():
            drain()

        return carry

    lax.fori_loop(0, 2, layer, 0)

    got(gt_ref.at[pl.ds(0, 15)], gsem.at[0])
    sent_weights(pairs)
    for s in range(2):
        got(w13.at[s], rw.at[s, 0])
        got(wdn.at[s], rw.at[s, 1])


def copy_blocks(*refs):
    for src, dst in zip(refs[:3], refs[3:]):
        dst[...] = src[...]


def hand_out(arrays):
    flat = [a.reshape(-1, a.shape[-1]) for a in arrays]
    specs = [pl.BlockSpec((a.shape[0] // COPY_STEPS, a.shape[1]), lambda i: (i, 0)) for a in flat]
    outs = pl.pallas_call(
        copy_blocks,
        grid=(COPY_STEPS,),
        out_shape=[jax.ShapeDtypeStruct(a.shape, a.dtype) for a in flat],
        in_specs=specs,
        out_specs=specs,
        compiler_params=pltpu.CompilerParams(vmem_limit_bytes=48_000_000),
    )(*flat)
    return tuple(o.reshape(a.shape) for o, a in zip(outs, arrays))


def solution(mesh):
    n_experts = mesh.shape["stage"] * mesh.shape["expert"]

    def per_device(gate_loc, up_loc, down_loc, x_loc, ids_loc, mix_loc):
        tok, width = x_loc.shape
        ff = gate_loc.shape[-1]
        half = width // 2
        chosen = ids_loc[..., None] == jnp.arange(n_experts)
        table = jnp.sum(jnp.where(chosen, mix_loc[..., None], 0.0), axis=2)
        table = jnp.transpose(table, (0, 2, 1)).reshape(16, 2, tok)
        table = jnp.pad(table, ((0, 0), (0, 6), (0, 0)))
        hbm = pl.BlockSpec(memory_space=pl.ANY)
        sds = jax.ShapeDtypeStruct
        outs = pl.pallas_call(
            functools.partial(moe_kernel, tok, width, ff),
            out_shape=(
                sds((2, 1, width, 2 * ff), BF16), sds((2, 1, ff, width), BF16), sds((2, tok, width), F32),
                sds((8, 2, tok, width), BF16),
                sds((8, 2, tok, half), F32), sds((8, 2, tok, half), F32),
                sds((4, 2, tok, half), F32), sds((2, 2, tok, half), F32), sds((2, 2, tok, half), F32), sds((2, 2, tok, half), F32),
            ),
            in_specs=[hbm] * 5,
            out_specs=(hbm,) * 10,
            scratch_shapes=[
                pltpu.VMEM((2, width, ff), BF16), pltpu.VMEM((2, width, ff), BF16), pltpu.VMEM((2, ff, width), BF16),
                pltpu.VMEM((tok, width), F32), pltpu.VMEM((tok, width), BF16),
                pltpu.VMEM((2, tok, width), BF16), pltpu.VMEM((2 * tok, ff), BF16),
                pltpu.VMEM((2, 2, 2, tok, half), F32), pltpu.VMEM((2, tok, half), F32),
                pltpu.VMEM((16, 8, tok), F32), pltpu.VMEM((2 * tok, min(128, tok)), F32), pltpu.VMEM((2, 2, tok, half), F32),
            ] + [pltpu.SemaphoreType.DMA(s) for s in (
                (3,), (5,), (3,), (2, 5), (2, 4), (2, 2), (2, 2), (2, 4), (1,),
                (2,), (8,), (4, 2), (4, 2), (2, 2), (2, 2), (2, 2), (2, 2), (2, WEIGHT_CHUNKS, 3), (2, 2))] + [pltpu.SemaphoreType.REGULAR],
            compiler_params=pltpu.CompilerParams(has_side_effects=True, vmem_limit_bytes=66_000_000),
        )(gate_loc, up_loc, down_loc, x_loc, table)
        return hand_out(outs[:3])

    weight_spec = P("stage", "expert")
    token_spec = P(None, FLAT)
    return jax.shard_map(per_device, mesh=mesh, in_specs=(weight_spec, weight_spec, weight_spec, P(FLAT), token_spec, token_spec), out_specs=(token_spec, token_spec, token_spec), check_vma=False)
```

```python
import functools

import jax
import jax.numpy as jnp
from jax import lax
from jax.experimental import pallas as pl
from jax.experimental.pallas import tpu as pltpu
from jax.sharding import PartitionSpec as P

NORM_EPS = 1e-6
FLAT = ("stage", "expert")
MESH = pl.DeviceIdType.MESH
F32 = jnp.float32
BF16 = jnp.bfloat16
WEIGHT_CHUNKS = 8
COPY_STEPS = 4
GAPS_STAY = (2,)
GAPS_LEAVE = (2, 3)
ORDER = ((0, 0), (0, 1), (1, 1), (1, 3), (1, 2), (0, 3), (0, 2), (1, 0))
STEP = {group: k for k, group in enumerate(ORDER)}
TABLE = sum((4 * d + cls) * 8 ** k for k, (d, cls) in enumerate(ORDER))


def flip(a, b):
    return a + b - 2 * a * b


def moe_kernel(tok, width, ff, w_gate, w_up, w_down, x_ref, gt_ref, w13, wdn, hid, u_all, s_loc, d2d, r1, r2, s_out, fin,
               wv_g, wv_u, wv_d, h, ub, ut, av, pp, ta, gall, gc, hs,
               wsem, lsem, gsem, us, up, ax, af, ap, az, dsend, drecv, s1, q1, s2, q2, so, hr, sw, rw, plane):
    half = width // 2
    tile_f = min(1024, ff)
    tile_d = min(1024, half)
    lanes = min(128, tok)
    z = lax.axis_index("stage")
    e = lax.axis_index("expert")
    y, x, c = e // 4, (e // 2) % 2, e % 2
    me = z * 8 + e
    ny, nx, nc, nz = 1 - y, 1 - x, 1 - c, 1 - z
    fy, fx = (1 - c) * y + c * ny, (1 - c) * nx + c * x
    sy, sx = c * y + (1 - c) * ny, c * nx + (1 - c) * x

    def dev(dz, dy, dx, dc):
        return (dz, dy * 4 + dx * 2 + dc)

    def group(gz, gy, gx):
        return gz * 4 + gy * 2 + gx

    def remote(src, dst, ssem, rsem, to):
        return pltpu.make_async_remote_copy(src_ref=src, dst_ref=dst, send_sem=ssem, recv_sem=rsem, device_id=to, device_id_type=MESH)

    def local(src, dst, sem):
        cp = pltpu.make_async_copy(src, dst, sem)
        cp.start()
        cp.wait()

    own_gate = pltpu.make_async_copy(gt_ref.at[me], gall.at[me], gsem.at[2])
    own_gate.start()

    def send_gate(off, carry):
        to = lax.rem(me + off, 16)
        remote(gt_ref.at[to], gall.at[me], gsem.at[0], gsem.at[1], (to // 8, lax.rem(to, 8))).start()
        return carry

    lax.fori_loop(1, 16, send_gate, 0)

    own_x = pltpu.make_async_copy(x_ref, ub, lsem.at[0])
    own_x.start()
    w_loads = [pltpu.make_async_copy(w_gate.at[0], wv_g, wsem.at[0]), pltpu.make_async_copy(w_up.at[0], wv_u, wsem.at[1]), pltpu.make_async_copy(w_down.at[0], wv_d, wsem.at[2])]
    own_x.wait()
    for load in w_loads:
        load.start()
    h[...] = ub[...].astype(F32)

    stays = (1 - flip(z, y)) * (1 - flip(y, x)) * (1 - flip(x, c))

    def weight_parts(k, q):
        rows = pl.ds(q * (width // WEIGHT_CHUNKS), width // WEIGHT_CHUNKS)
        rows_d = pl.ds(q * (ff // WEIGHT_CHUNKS), ff // WEIGHT_CHUNKS)
        return ((w_gate.at[0, k, rows], wv_g.at[k, rows], w13.at[z, 0, rows, pl.ds(0, ff)], 0),
                (w_up.at[0, k, rows], wv_u.at[k, rows], w13.at[z, 0, rows, pl.ds(ff, ff)], 0),
                (w_down.at[0, k, rows_d], wv_d.at[k, rows_d], wdn.at[z, 0, rows_d], 1))

    def stays_here(k):
        return jnp.logical_and(stays == 1, c == k)

    def weight_copies(k, q):
        return [remote(src, dst, sw.at[k, q, i], rw.at[z, kind], (y, x * 4 + c * 2 + k))
                for i, (src, _, dst, kind) in enumerate(weight_parts(k, q))]

    def send_weights(pairs):
        for k, q in pairs:
            @pl.when(stays_here(k))
            def _():
                for _, src, dst, kind in weight_parts(k, q):
                    pltpu.make_async_copy(src, dst, rw.at[z, kind]).start()

            @pl.when(jnp.logical_not(stays_here(k)))
            def _():
                for copy in weight_copies(k, q):
                    copy.start()

    def sent_weights(pairs):
        for k, q in pairs:
            @pl.when(jnp.logical_not(stays_here(k)))
            def _():
                for copy in weight_copies(k, q):
                    copy.wait_send()

    pairs = [(k, q) for q in range(WEIGHT_CHUNKS) for k in range(2)]
    leaves = flip(y, z) == 1

    def rows_load(gz, gy, gx):
        return pltpu.make_async_copy(u_all.at[group(gz, gy, gx)], ut, lsem.at[2])

    def gate_columns(gz, gy, gx):
        for b in range(2):
            flat = gz * 8 + gy * 4 + gx * 2 + b
            for j in range(tok // lanes):
                row = gall[flat, :, j * lanes:(j + 1) * lanes]
                gc[b * tok + j * lanes:b * tok + (j + 1) * lanes, :] = jnp.concatenate([row] * (lanes // 8), axis=0).T

    def expert(ex, slot):
        if True:
            def ff_tile(t, carry):
                cols = pl.ds(pl.multiple_of(t * tile_f, tile_f), tile_f)
                rows_u = ut[...].reshape(2 * tok, width)
                zg = jnp.dot(rows_u, wv_g[ex, :, cols], preferred_element_type=F32)
                zu = jnp.dot(rows_u, wv_u[ex, :, cols], preferred_element_type=F32)
                av[:, cols] = (jax.nn.silu(zg) * zu).astype(BF16)
                return carry

            lax.fori_loop(0, ff // tile_f, ff_tile, 0)

            def out_tile(t, carry):
                cols = pl.ds(pl.multiple_of(t * tile_d, tile_d), tile_d)
                side = t // (half // tile_d)
                at = pl.ds(pl.multiple_of(lax.rem(t, half // tile_d) * tile_d, tile_d), tile_d)
                o = jnp.dot(av[...], wv_d[ex, :, cols], preferred_element_type=F32).astype(BF16).astype(F32)
                gate = gc[:, ex:ex + 1]
                o = jnp.where(gate > 0, gate * o, 0.0)
                for b in range(2):
                    part = o[b * tok:(b + 1) * tok]
                    if ex:
                        part = part + pp[slot, side, b, :, at]
                    pp[slot, side, b, :, at] = part
                return carry

            lax.fori_loop(0, width // tile_d, out_tile, 0)

    def lane(gz, gy, gx):
        return u_all.at[group(gz, gy, gx), c]

    def lane_part(gz, gy, gx, which):
        return u_all.at[group(gz, gy, gx), c, pl.ds(which * (tok // 2), tok // 2)]

    def to_x(d, gz):
        return remote(lane(gz, y, x), lane(gz, y, x), ax.at[d, 0], us.at[d, 0], dev(z, y, nx, c))

    def to_y(d, gz):
        return remote(lane(gz, y, x), lane(gz, y, x), ax.at[d, 1], us.at[d, 1], dev(z, ny, x, c))

    def x_on(d, gz):
        return remote(lane_part(gz, y, nx, 0), lane_part(gz, y, nx, 0), af.at[d, 0], us.at[d, 2], dev(z, ny, x, c))

    def y_on(d, gz):
        return remote(lane_part(gz, ny, x, 1), lane_part(gz, ny, x, 1), af.at[d, 1], us.at[d, 3], dev(z, y, nx, c))

    def to_partner(d, gz, gy, gx, cls):
        return remote(lane(gz, gy, gx), lane(gz, gy, gx), ap.at[d, cls], up.at[d, cls], dev(z, y, x, nc))

    def got(dst, sem):
        pltpu.make_async_copy(dst, dst, sem).wait()

    def to_z(layer_dev):
        return remote(lane(z, y, x), lane(z, y, x), az.at[0], us.at[1, 4], dev(nz, y, x, c))

    def spread(d, gz):
        to_x(d, gz).start()
        to_y(d, gz).start()
        to_partner(d, gz, y, x, 0).start()

    def relay(d, gz):
        got(lane(gz, y, nx), us.at[d, 0])
        x_on(d, gz).start()
        to_partner(d, gz, y, nx, 1).start()
        got(lane(gz, ny, x), us.at[d, 1])
        y_on(d, gz).start()
        to_partner(d, gz, ny, x, 2).start()

    def corner(d, gz):
        got(lane_part(gz, ny, nx, 0), us.at[d, 2])
        got(lane_part(gz, ny, nx, 1), us.at[d, 3])
        to_partner(d, gz, ny, nx, 3).start()

    def d2d_copy(k, slot):
        return remote(pp.at[slot, nc], d2d.at[k], dsend.at[slot], drecv.at[k], dev(z, y, x, nc))

    def step_class(k):
        code = lax.rem(lax.div(jnp.int32(TABLE), lax.shift_left(jnp.int32(1), 3 * k)), 8)
        return code // 4, lax.rem(code // 2, 2), lax.rem(code, 2)

    def first_send(k, d, ds, b):
        return remote(s_loc.at[k, b], r1.at[d * 2 + ds, b], s1.at[d * 2 + ds, b], q1.at[d * 2 + ds, b], dev(z, fy, fx, c))

    def sum_load(k):
        return pltpu.make_async_copy(d2d.at[k], ta, lsem.at[3])

    def sum_store(k, slot):
        return pltpu.make_async_copy(pp.at[slot, c], s_loc.at[k], lsem.at[4])

    def add_partner(k, slot):
        sum_load(k).wait()
        for b in range(2):
            pp[slot, c, b] = pp[slot, c, b] + ta[b]
        sum_store(k, slot).start()

    def pass_on(k, slot):
        d, dy, dx = step_class(k)
        df = (1 - c) * dx + c * dy
        ds = (1 - c) * dy + c * dx
        sum_store(k, slot).wait()

        @pl.when(df == 1)
        def _():
            for b in range(2):
                first_send(k, d, ds, b).start()

    def second_send(d, b):
        return remote(s_out.at[d, b], r2.at[d, b], s2.at[d, b], q2.at[d, b], dev(z, sy, sx, c))

    def finish_second(d, b):
        k = c * STEP[d, 1] + (1 - c) * STEP[d, 2]
        load = pltpu.make_async_copy(s_loc.at[k, b], ta.at[0], lsem.at[0])
        load.start()
        got(r1.at[d * 2 + 1, b], q1.at[d * 2 + 1, b])
        local(r1.at[d * 2 + 1, b], ta.at[1], lsem.at[1])
        load.wait()
        ta[0] = ta[0] + ta[1]
        local(ta.at[0], s_out.at[d, b], lsem.at[0])
        second_send(d, b).start()

    def home_send(d, b):
        return remote(fin.at[d, b], hs.at[z, c], so.at[d, b], hr.at[z, c], dev(flip(z, d), y, x, b))

    def finish_own(d, b):
        load = pltpu.make_async_copy(s_loc.at[STEP[d, 0], b], ta.at[0], lsem.at[0])
        load.start()
        got(r1.at[d * 2, b], q1.at[d * 2, b])
        local(r1.at[d * 2, b], ta.at[1], lsem.at[1])
        load.wait()
        ta[0] = ta[0] + ta[1]
        got(r2.at[d, b], q2.at[d, b])
        local(r2.at[d, b], ta.at[1], lsem.at[1])
        ta[0] = ta[0] + ta[1]
        local(ta.at[0], fin.at[d, b], lsem.at[0])
        if d == 1:
            home_send(d, b).start()
        else:
            @pl.when(c == b)
            def _():
                pltpu.make_async_copy(fin.at[d, b], hs.at[z, c], hr.at[z, c]).start()

            @pl.when(c != b)
            def _():
                home_send(d, b).start()

    def active():
        spread(0, z)

        @pl.when(z == 0)
        def _():
            for load in w_loads:
                load.wait()

        own_gate.wait()
        got(gall.at[pl.ds(0, 15)], gsem.at[1])

        def step(k, carry):
            d, dy, dx = step_class(k)
            gz, gy, gx = flip(z, d), flip(y, dy), flip(x, dx)
            cls = dy * 2 + dx
            slot = lax.rem(k, 2)

            @pl.when(k == 1)
            def _():
                got(lane(nz, y, x), us.at[1, 4])
                spread(1, nz)

            for dd in range(2):
                @pl.when(k == max(1, min(STEP[dd, 1], STEP[dd, 2])))
                def _():
                    relay(dd, flip(z, dd))

                @pl.when(k == STEP[dd, 3])
                def _():
                    corner(dd, flip(z, dd))

            for mine, gaps in ((jnp.logical_not(leaves), GAPS_STAY), (leaves, GAPS_LEAVE)):
                for pair, at in zip(pairs, gaps):
                    @pl.when(jnp.logical_and(mine, k == at))
                    def _():
                        send_weights([pair])

            got(u_all.at[group(gz, gy, gx), nc], up.at[d, cls])
            rows_load(gz, gy, gx).start()
            gate_columns(gz, gy, gx)

            @pl.when(k >= 2)
            def _():
                pass_on(k - 2, slot)
                d2d_copy(k - 2, slot).wait_send()

            rows_load(gz, gy, gx).wait()
            expert(0, slot)

            @pl.when(k == 7)
            def _():
                for b in range(2):
                    finish_second(1, b)

            @pl.when(k >= 1)
            def _():
                got(d2d.at[k - 1], drecv.at[k - 1])
                sum_load(k - 1).start()

            expert(1, slot)

            @pl.when(k >= 1)
            def _():
                add_partner(k - 1, 1 - slot)

            d2d_copy(k, slot).start()
            return carry

        lax.fori_loop(0, 8, step, 0)
        pass_on(6, 0)
        got(d2d.at[7], drecv.at[7])
        sum_load(7).start()
        add_partner(7, 1)
        pass_on(7, 1)
        for b in range(2):
            finish_second(0, b)
        for b in range(2):
            finish_own(1, b)
        for b in range(2):
            finish_own(0, b)

    def drain():
        for d in range(2):
            gz = flip(z, d)
            to_x(d, gz).wait_send()
            to_y(d, gz).wait_send()
            x_on(d, gz).wait_send()
            y_on(d, gz).wait_send()
            for cls in range(4):
                to_partner(d, gz, flip(y, cls // 2), flip(x, cls % 2), cls).wait_send()
            d2d_copy(6 + d, d).wait_send()
            for b in range(2):
                for ds in range(2):
                    first_send(0, d, ds, b).wait_send()
                second_send(d, b).wait_send()
            for b in range(2):
                if d == 1:
                    home_send(d, b).wait_send()
                else:
                    @pl.when(c != b)
                    def _():
                        home_send(d, b).wait_send()

    def layer(l, carry):
        rows = min(32, tok)

        def norm(i, cc):
            r = pl.ds(pl.multiple_of(i * rows, rows), rows)
            v = h[r, :]
            ub[r, :] = (v * lax.rsqrt(jnp.mean(v * v, axis=-1, keepdims=True) + NORM_EPS)).astype(BF16)
            return cc

        lax.fori_loop(0, tok // rows, norm, 0)
        local(ub, lane(z, y, x), lsem.at[0])

        @pl.when(z != l)
        def _():
            to_z(l).start()

            @pl.when(z == 1)
            def _():
                for load in w_loads:
                    load.wait()

            @pl.when(jnp.logical_not(leaves))
            def _():
                send_weights(pairs[len(GAPS_STAY):])

            to_z(l).wait_send()
            for i in range(1, 8):
                pl.semaphore_signal(plane, inc=1, device_id=(z, lax.rem(e + i, 8)), device_id_type=MESH)
            pl.semaphore_wait(plane, 7)

            @pl.when(leaves)
            def _():
                send_weights(pairs[len(GAPS_LEAVE):])

        @pl.when(z == l)
        def _():
            active()

        for s in range(2):
            got(hs.at[l, s], hr.at[l, s])
            h[:, s * half:(s + 1) * half] = h[:, s * half:(s + 1) * half] + hs[l, s]
        local(h, hid.at[l], lsem.at[0])

        @pl.when(z == l)
        def _():
            drain()

        return carry

    lax.fori_loop(0, 2, layer, 0)

    got(gt_ref.at[pl.ds(0, 15)], gsem.at[0])
    sent_weights(pairs)
    for s in range(2):
        got(w13.at[s], rw.at[s, 0])
        got(wdn.at[s], rw.at[s, 1])


def copy_blocks(*refs):
    for src, dst in zip(refs[:3], refs[3:]):
        dst[...] = src[...]


def hand_out(arrays):
    flat = [a.reshape(-1, a.shape[-1]) for a in arrays]
    specs = [pl.BlockSpec((a.shape[0] // COPY_STEPS, a.shape[1]), lambda i: (i, 0)) for a in flat]
    outs = pl.pallas_call(
        copy_blocks,
        grid=(COPY_STEPS,),
        out_shape=[jax.ShapeDtypeStruct(a.shape, a.dtype) for a in flat],
        in_specs=specs,
        out_specs=specs,
        compiler_params=pltpu.CompilerParams(vmem_limit_bytes=48_000_000),
    )(*flat)
    return tuple(o.reshape(a.shape) for o, a in zip(outs, arrays))


def solution(mesh):
    n_experts = mesh.shape["stage"] * mesh.shape["expert"]

    def per_device(gate_loc, up_loc, down_loc, x_loc, ids_loc, mix_loc):
        tok, width = x_loc.shape
        ff = gate_loc.shape[-1]
        half = width // 2
        chosen = ids_loc[..., None] == jnp.arange(n_experts)
        table = jnp.sum(jnp.where(chosen, mix_loc[..., None], 0.0), axis=2)
        table = jnp.transpose(table, (0, 2, 1)).reshape(16, 2, tok)
        table = jnp.pad(table, ((0, 0), (0, 6), (0, 0)))
        hbm = pl.BlockSpec(memory_space=pl.ANY)
        sds = jax.ShapeDtypeStruct
        outs = pl.pallas_call(
            functools.partial(moe_kernel, tok, width, ff),
            out_shape=(
                sds((2, 1, width, 2 * ff), BF16), sds((2, 1, ff, width), BF16), sds((2, tok, width), F32),
                sds((8, 2, tok, width), BF16),
                sds((8, 2, tok, half), F32), sds((8, 2, tok, half), F32),
                sds((4, 2, tok, half), F32), sds((2, 2, tok, half), F32), sds((2, 2, tok, half), F32), sds((2, 2, tok, half), F32),
            ),
            in_specs=[hbm] * 5,
            out_specs=(hbm,) * 10,
            scratch_shapes=[
                pltpu.VMEM((2, width, ff), BF16), pltpu.VMEM((2, width, ff), BF16), pltpu.VMEM((2, ff, width), BF16),
                pltpu.VMEM((tok, width), F32), pltpu.VMEM((tok, width), BF16),
                pltpu.VMEM((2, tok, width), BF16), pltpu.VMEM((2 * tok, ff), BF16),
                pltpu.VMEM((2, 2, 2, tok, half), F32), pltpu.VMEM((2, tok, half), F32),
                pltpu.VMEM((16, 8, tok), F32), pltpu.VMEM((2 * tok, min(128, tok)), F32), pltpu.VMEM((2, 2, tok, half), F32),
            ] + [pltpu.SemaphoreType.DMA(s) for s in (
                (3,), (5,), (3,), (2, 5), (2, 4), (2, 2), (2, 2), (2, 4), (1,),
                (2,), (8,), (4, 2), (4, 2), (2, 2), (2, 2), (2, 2), (2, 2), (2, WEIGHT_CHUNKS, 3), (2, 2))] + [pltpu.SemaphoreType.REGULAR],
            compiler_params=pltpu.CompilerParams(has_side_effects=True, vmem_limit_bytes=66_000_000),
        )(gate_loc, up_loc, down_loc, x_loc, table)
        return hand_out(outs[:3])

    weight_spec = P("stage", "expert")
    token_spec = P(None, FLAT)
    return jax.shard_map(per_device, mesh=mesh, in_specs=(weight_spec, weight_spec, weight_spec, P(FLAT), token_spec, token_spec), out_specs=(token_spec, token_spec, token_spec), check_vma=False)
```
